8 devices in a mesh: dp: 2 (over z, y), tp: 4 (over x, core).
Axes of the slice: x: 2, y: 2, z: 1, core: 2. Of those that a mesh axis runs over, the one named last changes fastest.
Arguments:
- tokens: int32 [4, 2048], P('dp')
- emb_table: bfloat16 [65536, 3072], P('tp')
- w_norm: float32 [3072], replicated
- dy_norm: bfloat16 [4, 2048, 3072], P('dp', 'tp')
- dy_resid: bfloat16 [4, 2048, 3072], P('dp', 'tp')
Outputs:
- output 1: bfloat16 [4, 2048, 3072], P('dp', 'tp')
- output 2: bfloat16 [4, 2048, 3072], P('dp', 'tp')
- output 3: float32 [65536, 3072], P(('tp', 'dp'))
- output 4: float32 [3072], replicated
All inputs are finite; a program needn't handle non-finite values.
Results may differ from the reference program's by a relative error of at most 0.00840549.
Values sent between devices are 32-bit elements.
A program may use at most 1 GiB of HBM per device.

```python
import jax
import jax.numpy as jnp
from jax import lax

VOCAB_ROWS = 65536
MODEL_DIM = 3072
NUM_SEQS = 4
SEQ_LEN = 2048
NORM_EPS = 1e-6
LOG_VOCAB = (VOCAB_ROWS - 1).bit_length()


def draw_tokens(key):
    k_level, k_ident, k_pick, k_flat = jax.random.split(key, 4)
    tok_shape = (NUM_SEQS, SEQ_LEN)
    zipf_level = jax.random.randint(k_level, tok_shape, 0, LOG_VOCAB + 1, dtype=jnp.int32)
    level_top = jnp.minimum(jnp.left_shift(jnp.ones(tok_shape, jnp.int32), zipf_level), VOCAB_ROWS)
    zipf_ids = jax.random.randint(k_ident, tok_shape, 0, level_top, dtype=jnp.int32)
    flat_ids = jax.random.randint(k_flat, tok_shape, 0, VOCAB_ROWS, dtype=jnp.int32)
    mix_pick = jax.random.randint(k_pick, tok_shape, 0, 4, dtype=jnp.int32)
    token_ids = jnp.where(mix_pick == 0, flat_ids, zipf_ids)
    return token_ids.at[0, 0].set(VOCAB_ROWS - 1)


def setup_inputs(seed: int = 0) -> dict:
    k_tok, k_tab, k_gain, k_norm, k_resid = jax.random.split(jax.random.key(seed), 5)
    tokens = draw_tokens(k_tok)
    emb_table = (jax.random.normal(k_tab, (VOCAB_ROWS, MODEL_DIM), jnp.float32) * MODEL_DIM ** -0.5).astype(jnp.bfloat16)
    w_norm = 0.6 * jax.random.normal(k_gain, (MODEL_DIM,), jnp.float32)
    dy_norm = jax.random.normal(k_norm, (NUM_SEQS, SEQ_LEN, MODEL_DIM), jnp.float32).astype(jnp.bfloat16)
    dy_resid = jax.random.normal(k_resid, (NUM_SEQS, SEQ_LEN, MODEL_DIM), jnp.float32).astype(jnp.bfloat16)
    return {"tokens": tokens, "emb_table": emb_table, "w_norm": w_norm, "dy_norm": dy_norm, "dy_resid": dy_resid}


def reference(tokens, emb_table, w_norm, dy_norm, dy_resid):
    emb_scale = jnp.asarray(MODEL_DIM ** 0.5, jnp.bfloat16)
    x_emb = emb_table[tokens] * emb_scale
    x_float = x_emb.astype(jnp.float32)
    inv_rms = lax.rsqrt(jnp.mean(x_float * x_float, axis=-1, keepdims=True) + NORM_EPS)
    x_hat = x_float * inv_rms
    norm_gain = 1.0 + w_norm
    y_norm = (x_hat * norm_gain).astype(jnp.bfloat16)
    dy_float = dy_norm.astype(jnp.float32)
    dx_hat = dy_float * norm_gain
    tok_grad = dy_resid.astype(jnp.float32) + inv_rms * (dx_hat - x_hat * jnp.mean(dx_hat * x_hat, axis=-1, keepdims=True))
    w_grad = jnp.sum(dy_float * x_hat, axis=(0, 1))
    emb_grad = jax.ops.segment_sum(tok_grad.reshape(-1, MODEL_DIM), tokens.reshape(-1), num_segments=VOCAB_ROWS) * emb_scale.astype(jnp.float32)
    return x_emb, y_norm, emb_grad, w_grad
```

```python
import functools
import math

import jax
import jax.numpy as jnp
import numpy as np
from jax import lax
from jax.experimental import pallas as pl
from jax.experimental.pallas import tpu as pltpu
from jax.sharding import PartitionSpec as P

NORM_EPS = 1e-6
LANES = 128
GATHER_ROWS = 16
TOKEN_BLOCK = 128
TOKEN_GROUP = 16
OUT_BLOCK = 512
SUM_ROWS = 8
COPY_ROWS = 16
SIZES = (32, 64, 96, 128, 192, 256, 320, 384, 448, 512, 576, 640, 768)
VMEM_LIMIT = 60 * 1024 * 1024


def count_below(values, edges):
    return jnp.sum((values[:, :, None] < edges[None, None, :]).astype(jnp.int32), axis=1)


def chunk_table(starts, lens, size, most):
    per_run = (lens + size - 1) // size
    upto = jnp.cumsum(per_run)
    before = upto - per_run
    chunk = jnp.arange(most, dtype=jnp.int32)
    hit = (chunk[:, None] >= before[None, :]) & (chunk[:, None] < upto[None, :])
    done = size * (chunk[:, None] - before[None, :])
    cut = [jnp.sum(jnp.where(hit, start[None, :] + done, 0), axis=1) for start in starts]
    left = jnp.sum(jnp.where(hit, lens[None, :] - done, 0), axis=1)
    return cut, jnp.clip(left, 0, size), upto


def lookup_exchange_kernel(core, size, stride, most, sent_ref, got_ref, send_sems, recv_sems):
    tp = lax.axis_index("tp")
    mine = lax.rem(tp, 2)
    region = pl.ds((tp // 2) * most, size)

    def copy(hop):
        peer = tp + hop - 2 * (tp & hop)
        return pltpu.make_async_remote_copy(
            src_ref=sent_ref.at[pl.ds(peer * stride, size)],
            dst_ref=got_ref.at[region],
            send_sem=send_sems.at[hop - 1],
            recv_sem=recv_sems.at[hop - 1],
            device_id={"tp": peer},
            device_id_type=pl.DeviceIdType.MESH,
        )

    @pl.when(mine == core)
    def _():
        for hop in (2, 3, 1):
            copy(hop).start()
        for hop in (1, 2, 3):
            copy(hop).wait_send()
        copy(2).wait_recv()

    @pl.when(mine != core)
    def _():
        for hop in (1, 3):
            copy(hop).wait_recv()


def grad_exchange_kernel(core, size, stride, most, num_tp, sums_ref, got_ref, send_sems, recv_sems):
    dp, tp = lax.axis_index("dp"), lax.axis_index("tp")
    mine = lax.rem(tp, 2)
    me = dp * num_tp + tp

    def copy(hop_x, hop_y, source):
        peer_x = tp // 2 + hop_x - 2 * ((tp // 2) & hop_x)
        peer_tp = peer_x * 2 + core
        peer_dp = dp + hop_y - 2 * (dp & hop_y)
        return pltpu.make_async_remote_copy(
            src_ref=sums_ref.at[pl.ds((peer_tp * 2 + peer_dp) * stride, size)],
            dst_ref=got_ref.at[pl.ds(source * most, size)],
            send_sem=send_sems.at[hop_y * 2 + hop_x],
            recv_sem=recv_sems.at[source],
            device_id={"dp": peer_dp, "tp": peer_tp},
            device_id_type=pl.DeviceIdType.MESH,
        )

    for hop_x, hop_y in ((1, 1), (1, 0), (0, 1)):
        copy(hop_x, hop_y, me).start()

    @pl.when(mine != core)
    def _():
        copy(0, 0, me).start()

    for hop_x, hop_y in ((1, 1), (1, 0), (0, 1)):
        copy(hop_x, hop_y, me).wait_send()

    @pl.when(mine != core)
    def _():
        copy(0, 0, me).wait_send()

    @pl.when(mine == core)
    def _():
        for source in range(2 * num_tp):

            @pl.when(source != me)
            def _():
                copy(1, 1, source).wait_recv()


def by_size(kernel, needed, sizes, rows, name, sems, operand):
    def branch(size):
        def call(held):
            return pl.pallas_call(
                functools.partial(kernel, size),
                out_shape=jax.ShapeDtypeStruct((rows,) + held.shape[1:], held.dtype),
                in_specs=[pl.BlockSpec(memory_space=pl.ANY)],
                out_specs=pl.BlockSpec(memory_space=pl.ANY),
                scratch_shapes=[pltpu.SemaphoreType.DMA((sems[0],)), pltpu.SemaphoreType.DMA((sems[1],))],
                compiler_params=pltpu.CompilerParams(has_side_effects=True),
                name=f"{name}_{size}",
            )(held)

        return call

    which = jnp.sum((needed > jnp.asarray(sizes, jnp.int32)).astype(jnp.int32))
    return lax.switch(which, [branch(size) for size in sizes], operand)


def gather_kernel(scale, wide, row_ref, src_ref, dst_ref, num_ref, table_ref, out_ref, slots, spread, stage, in_sems, out_sems):
    num = num_ref[0]

    def fetch(chunk):
        slot = lax.rem(chunk, 2)
        src = src_ref[chunk]
        for i in range(GATHER_ROWS):
            first = pl.multiple_of((row_ref[src + i] // 8) * 8, 8)
            pltpu.make_async_copy(table_ref.at[pl.ds(first, 8), :], slots.at[slot, i], in_sems.at[slot]).start()

    def put(chunk):
        slot = lax.rem(chunk, 2)
        return pltpu.make_async_copy(stage.at[slot], out_ref.at[pl.ds(dst_ref[chunk], GATHER_ROWS)], out_sems.at[slot])

    @pl.when(num > 0)
    def _():
        fetch(0)

    def body(chunk, _):
        slot = lax.rem(chunk, 2)

        @pl.when(chunk + 1 < num)
        def _():
            fetch(chunk + 1)

        pltpu.make_async_copy(slots.at[1 - slot], slots.at[slot], in_sems.at[slot]).wait()

        @pl.when(chunk >= 2)
        def _():
            put(chunk - 2).wait()

        src = src_ref[chunk]
        for i in range(GATHER_ROWS):
            for k in range(wide):
                spread[i, 8 * k : 8 * k + 8, :] = slots[slot, i, :, k * LANES : (k + 1) * LANES].astype(jnp.float32)
            row = lax.rem(row_ref[src + i], 8)
            stage[slot, i] = spread[i, pl.ds(row, wide, stride=8), :] * scale
        put(chunk).start()
        return 0

    lax.fori_loop(0, num, body, 0)

    @pl.when(num >= 2)
    def _():
        put(num - 2).wait()

    @pl.when(num >= 1)
    def _():
        put(num - 1).wait()


def token_kernel(wide, num_tp, most, stride, pos_ref, seg_ref, own_ref, sent_ref, got0_ref, got1_ref, w_ref, dyn_ref, dyr_ref, xe_ref, y_ref, sums_ref, wg_ref, held, total, grid_x, grid_g, wsum, sems):
    step = pl.program_id(0)
    steps = pl.num_programs(0)
    dim = wide * LANES
    num_own = 2 * num_tp

    def load_all(act):
        for p in range(num_tp):
            got = got1_ref if p % 2 else got0_ref

            def one(i, _):
                to = held.at[pl.ds(seg_ref[num_tp + p] + i * COPY_ROWS, COPY_ROWS)]

                @pl.when(own_ref[0] == p)
                def _():
                    act(pltpu.make_async_copy(sent_ref.at[pl.ds(p * stride + i * COPY_ROWS, COPY_ROWS)], to, sems.at[0]))

                @pl.when(own_ref[0] != p)
                def _():
                    act(pltpu.make_async_copy(got.at[pl.ds((p // 2) * most + i * COPY_ROWS, COPY_ROWS)], to, sems.at[0]))

                return 0

            lax.fori_loop(0, seg_ref[p], one, 0)

    def store_all(act):
        for o in range(num_own):

            def one(i, _):
                at = total.at[pl.ds(seg_ref[2 * num_tp + num_own + o] + i * COPY_ROWS, COPY_ROWS)]
                act(pltpu.make_async_copy(at, sums_ref.at[pl.ds(o * stride + i * COPY_ROWS, COPY_ROWS)], sems.at[0]))
                return 0

            lax.fori_loop(0, seg_ref[2 * num_tp + o], one, 0)

    @pl.when(step == 0)
    def _():
        load_all(lambda copy: copy.start())

        def clear(i, _):
            for j in range(8):
                total[i * 8 + j] = jnp.zeros((wide, LANES), jnp.float32)
            return 0

        lax.fori_loop(0, total.shape[0] // 8, clear, 0)
        wsum[...] = jnp.zeros_like(wsum)
        load_all(lambda copy: copy.wait())

    def group(index, _):
        base = step * TOKEN_BLOCK + index * TOKEN_GROUP
        rows = pl.ds(pl.multiple_of(index * TOKEN_GROUP, TOKEN_GROUP), TOKEN_GROUP)
        where = [pos_ref[base + j] for j in range(TOKEN_GROUP)]
        for j in range(TOKEN_GROUP):
            grid_x[pl.ds(j, wide, stride=TOKEN_GROUP), :] = held[where[j]]
        tile = [slice(TOKEN_GROUP * k, TOKEN_GROUP * (k + 1)) for k in range(wide)]
        lane = [slice(LANES * k, LANES * (k + 1)) for k in range(wide)]
        square = jnp.zeros((TOKEN_GROUP, LANES), jnp.float32)
        for k in range(wide):
            xe = grid_x[tile[k], :].astype(jnp.bfloat16)
            xe_ref[rows, lane[k]] = xe
            x = xe.astype(jnp.float32)
            grid_x[tile[k], :] = x
            square += x * x
        inv = lax.rsqrt(jnp.sum(square, axis=1, keepdims=True) * (1.0 / dim) + NORM_EPS)
        inner = jnp.zeros((TOKEN_GROUP, LANES), jnp.float32)
        for k in range(wide):
            xh = grid_x[tile[k], :] * inv
            grid_x[tile[k], :] = xh
            gain = 1.0 + w_ref[0:1, lane[k]]
            inner += dyn_ref[rows, lane[k]].astype(jnp.float32) * gain * xh
        mean = jnp.sum(inner, axis=1, keepdims=True) * (1.0 / dim)
        for k in range(wide):
            xh = grid_x[tile[k], :]
            gain = 1.0 + w_ref[0:1, lane[k]]
            dy = dyn_ref[rows, lane[k]].astype(jnp.float32)
            y_ref[rows, lane[k]] = (xh * gain).astype(jnp.bfloat16)
            wsum[:, lane[k]] += dy * xh
            grid_g[tile[k], :] = dyr_ref[rows, lane[k]].astype(jnp.float32) + inv * (dy * gain - xh * mean)
        for j in range(TOKEN_GROUP):
            total[where[j]] += grid_g[pl.ds(j, wide, stride=TOKEN_GROUP), :]
        return 0

    lax.fori_loop(0, TOKEN_BLOCK // TOKEN_GROUP, group, 0)

    @pl.when(step == steps - 1)
    def _():
        wg_ref[...] = jnp.sum(wsum[...], axis=0, keepdims=True)
        store_all(lambda copy: copy.start())
        store_all(lambda copy: copy.wait())


def sum_kernel(scale, wide, depth, upto_ref, src_ref, at_ref, cnt_ref, place_ref, own_ref, sums_ref, got0_ref, got1_ref, out_ref, acc, ring, sems):
    block = pl.program_id(0)
    num = upto_ref[pl.num_programs(0)]
    spare = (OUT_BLOCK // 8) * wide * 8

    def fetch(chunk):
        slot = lax.rem(chunk, depth)
        src = src_ref[chunk]

        @pl.when(src < own_ref[1])
        def _():
            @pl.when(own_ref[0] == 0)
            def _():
                pltpu.make_async_copy(got0_ref.at[pl.ds(src, SUM_ROWS)], ring.at[slot], sems.at[slot]).start()

            @pl.when(own_ref[0] != 0)
            def _():
                pltpu.make_async_copy(got1_ref.at[pl.ds(src, SUM_ROWS)], ring.at[slot], sems.at[slot]).start()

        @pl.when(src >= own_ref[1])
        def _():
            pltpu.make_async_copy(sums_ref.at[pl.ds(src - own_ref[1], SUM_ROWS)], ring.at[slot], sems.at[slot]).start()

    @pl.when(block == 0)
    def _():
        for c in range(depth - 1):

            @pl.when(c < num)
            def _():
                fetch(c)

        def clear(i, _):
            acc[pl.ds(pl.multiple_of(i * wide * 8, 8), wide * 8), :] = jnp.zeros((wide * 8, LANES), jnp.float32)
            return 0

        lax.fori_loop(0, OUT_BLOCK // 8 + 1, clear, 0)

    def body(chunk, _):
        slot = lax.rem(chunk, depth)
        pltpu.make_async_copy(got0_ref.at[pl.ds(0, SUM_ROWS)], ring.at[slot], sems.at[slot]).wait()

        @pl.when(chunk + depth - 1 < num)
        def _():
            fetch(chunk + depth - 1)

        src, cnt = at_ref[chunk], cnt_ref[chunk]
        for i in range(SUM_ROWS):
            at = pl.ds(jnp.where(i < cnt, place_ref[src + i], spare), wide, stride=8)
            acc[at, :] += ring[slot, i]
        return 0

    lax.fori_loop(upto_ref[block], upto_ref[block + 1], body, 0)

    def put(i, _):
        rows = pl.ds(pl.multiple_of(i * 8, 8), 8)
        for k in range(wide):
            at = pl.ds(pl.multiple_of(i * wide * 8 + 8 * k, 8), 8)
            out_ref[rows, k * LANES : (k + 1) * LANES] = acc[at, :] * scale
            acc[at, :] = jnp.zeros((8, LANES), jnp.float32)
        return 0

    lax.fori_loop(0, OUT_BLOCK // 8, put, 0)


def solution(mesh):
    num_dp, num_tp = mesh.shape["dp"], mesh.shape["tp"]
    num_dev = num_dp * num_tp

    def local_step(tokens, emb_table, w_norm, dy_norm, dy_resid):
        shard_rows, dim = emb_table.shape
        seqs, span = dy_norm.shape[:2]
        held_rows = seqs * span
        wide = dim // LANES
        vocab = shard_rows * num_tp
        own_rows = shard_rows // num_dp
        scale = float(np.float32(math.sqrt(dim)).astype(jnp.bfloat16))
        dp, tp = lax.axis_index("dp"), lax.axis_index("tp")
        any_space = pl.BlockSpec(memory_space=pl.ANY)
        smem = pl.BlockSpec(memory_space=pltpu.SMEM)

        everyone = lax.all_gather(tokens, "dp", axis=0, tiled=True)
        ids = everyone.reshape(num_dp, seqs, num_tp, span).transpose(0, 2, 1, 3).reshape(num_dev, held_rows)
        ordered = jnp.sort(ids, axis=1)
        again = jnp.concatenate([jnp.zeros((num_dev, 1), bool), ordered[:, 1:] == ordered[:, :-1]], axis=1)
        uniq = jnp.sort(jnp.where(again, vocab, ordered), axis=1)
        edges = jnp.arange(num_dev + 1, dtype=jnp.int32) * own_rows
        cuts = count_below(uniq, edges)
        shard_cuts = cuts[:, ::num_dp]
        me, own = dp * num_tp + tp, tp * num_dp + dp
        device = jnp.arange(num_dev, dtype=jnp.int32)

        looked = shard_cuts[:, 1:] - shard_cuts[:, :-1]
        looked = jnp.where(jnp.arange(num_tp)[None, :] == (device % num_tp)[:, None], 0, looked)
        owned = cuts[:, 1:] - cuts[:, :-1]
        owned = jnp.where(device[None, :] == ((device % num_tp) * num_dp + device // num_tp)[:, None], 0, owned)
        look_need = [jnp.max(looked[:, core::2]) for core in range(2)]
        grad_need = [jnp.max(owned.reshape(num_dev, num_tp, num_dp)[:, core::2]) for core in range(2)]
        sizes = [size for size in SIZES if size < held_rows] + [held_rows]

        group = dp * num_tp + jnp.arange(num_tp, dtype=jnp.int32)
        group_cuts = lax.dynamic_slice_in_dim(shard_cuts, dp * num_tp, num_tp, 0)
        lo = lax.dynamic_index_in_dim(group_cuts, tp, 1, keepdims=False)
        size = lax.dynamic_index_in_dim(group_cuts, tp + 1, 1, keepdims=False) - lo
        stride = held_rows + GATHER_ROWS
        most = num_tp * (held_rows // GATHER_ROWS) + num_tp
        lane_of = jnp.arange(num_tp, dtype=jnp.int32)
        (src, dst), _, upto = chunk_table([group * held_rows + lo, lane_of * stride], size, GATHER_ROWS, most)
        listed = jnp.clip(uniq - tp * shard_rows, 0, shard_rows - 1).reshape(-1)
        listed = jnp.pad(listed, (0, GATHER_ROWS))
        sent = pl.pallas_call(
            functools.partial(gather_kernel, scale, wide),
            out_shape=jax.ShapeDtypeStruct((num_tp * stride, wide, LANES), jnp.float32),
            in_specs=[smem] * 4 + [any_space],
            out_specs=any_space,
            scratch_shapes=[
                pltpu.VMEM((2, GATHER_ROWS, 8, dim), jnp.bfloat16),
                pltpu.VMEM((GATHER_ROWS, wide * 8, LANES), jnp.float32),
                pltpu.VMEM((2, GATHER_ROWS, wide, LANES), jnp.float32),
                pltpu.SemaphoreType.DMA((2,)),
                pltpu.SemaphoreType.DMA((2,)),
            ],
            compiler_params=pltpu.CompilerParams(vmem_limit_bytes=16 * 1024 * 1024),
            name="gather",
        )(listed, src, dst, upto[-1:], emb_table)
        rows = []
        for core in range(2):

            def look(size, *refs, core=core):
                lookup_exchange_kernel(core, size, stride, held_rows, *refs)

            rows.append(by_size(look, look_need[core], sizes, num_tp // 2 * held_rows, f"lookup{core}", (3, 3), sent))

        my_uniq = lax.dynamic_index_in_dim(uniq, me, 0, keepdims=False)
        my_ids = lax.dynamic_index_in_dim(ids, me, 0, keepdims=False)
        my_cuts = lax.dynamic_index_in_dim(cuts, me, 0, keepdims=False)
        place = jnp.sum((my_uniq[None, :] < my_ids[:, None]).astype(jnp.int32), axis=1)
        seg_lo = my_cuts[:-1:num_dp]
        seg_copies = (my_cuts[num_dp::num_dp] - seg_lo + COPY_ROWS - 1) // COPY_ROWS
        seg_base = (jnp.cumsum(seg_copies) - seg_copies) * COPY_ROWS
        shift = seg_base - seg_lo
        pos = place + jnp.sum(jnp.where((my_ids // shard_rows)[:, None] == lane_of[None, :], shift[None, :], 0), axis=1)
        own_copies = (my_cuts[1:] - my_cuts[:-1] + COPY_ROWS - 1) // COPY_ROWS
        own_base = my_cuts[:-1] + jnp.repeat(shift, num_dp)
        segments = jnp.concatenate([seg_copies, seg_base, own_copies, own_base])
        token_spec = pl.BlockSpec((TOKEN_BLOCK, dim), lambda i: (i, 0))
        act = jax.ShapeDtypeStruct((held_rows, dim), jnp.bfloat16)
        kept = held_rows + (num_tp + 1) * COPY_ROWS
        x_emb, y_norm, sums, w_part = pl.pallas_call(
            functools.partial(token_kernel, wide, num_tp, held_rows, stride),
            grid=(held_rows // TOKEN_BLOCK,),
            out_shape=[act, act, jax.ShapeDtypeStruct((num_dev * stride, wide, LANES), jnp.float32), jax.ShapeDtypeStruct((1, dim), jnp.float32)],
            in_specs=[smem] * 3 + [any_space] * 3 + [pl.BlockSpec((1, dim), lambda i: (0, 0)), token_spec, token_spec],
            out_specs=[token_spec, token_spec, any_space, pl.BlockSpec((1, dim), lambda i: (0, 0))],
            scratch_shapes=[
                pltpu.VMEM((kept, wide, LANES), jnp.float32),
                pltpu.VMEM((kept, wide, LANES), jnp.float32),
                pltpu.VMEM((TOKEN_GROUP * wide, LANES), jnp.float32),
                pltpu.VMEM((TOKEN_GROUP * wide, LANES), jnp.float32),
                pltpu.VMEM((TOKEN_GROUP, dim), jnp.float32),
                pltpu.SemaphoreType.DMA((1,)),
            ],
            compiler_params=pltpu.CompilerParams(vmem_limit_bytes=VMEM_LIMIT),
            name="tokens",
        )(pos, segments, tp.reshape(1), sent, *rows, w_norm.reshape(1, dim), dy_norm.reshape(held_rows, dim), dy_resid.reshape(held_rows, dim))
        w_grad = lax.psum(w_part.reshape(dim), ("dp", "tp"))

        got = []
        for core in range(2):

            def give(size, *refs, core=core):
                grad_exchange_kernel(core, size, stride, held_rows, num_tp, *refs)

            got.append(by_size(give, grad_need[core], sizes, num_dev * held_rows + SUM_ROWS, f"grads{core}", (4, num_dev), sums))

        blocks = own_rows // OUT_BLOCK
        marks = own * own_rows + jnp.arange(blocks + 1, dtype=jnp.int32) * OUT_BLOCK
        fence = count_below(uniq, marks)
        local = num_dev * held_rows + SUM_ROWS
        first = jnp.where(device == me, local + own * stride, device * held_rows)
        run_at = (device[:, None] * held_rows + fence[:, :-1]).T.reshape(-1)
        run_src = (first[:, None] + fence[:, :-1] - fence[:, :1]).T.reshape(-1)
        run_len = (fence[:, 1:] - fence[:, :-1]).T.reshape(-1)
        most = num_dev * held_rows // SUM_ROWS + blocks * num_dev
        (src, at), cnt, upto = chunk_table([run_src, run_at], run_len, SUM_ROWS, most)
        upto = jnp.concatenate([jnp.zeros((1,), jnp.int32), upto[num_dev - 1 :: num_dev]])
        inside = uniq.reshape(-1) & (OUT_BLOCK - 1)
        place = jnp.pad((inside >> 3) * (wide * 8) + (inside & 7), (0, SUM_ROWS))
        depth = 8
        emb_grad = pl.pallas_call(
            functools.partial(sum_kernel, scale, wide, depth),
            grid=(blocks,),
            out_shape=jax.ShapeDtypeStruct((own_rows, dim), jnp.float32),
            in_specs=[smem] * 6 + [any_space] * 3,
            out_specs=pl.BlockSpec((OUT_BLOCK, dim), lambda i: (i, 0)),
            scratch_shapes=[
                pltpu.VMEM(((OUT_BLOCK // 8 + 1) * wide * 8, LANES), jnp.float32),
                pltpu.VMEM((depth, SUM_ROWS, wide, LANES), jnp.float32),
                pltpu.SemaphoreType.DMA((depth,)),
            ],
            compiler_params=pltpu.CompilerParams(vmem_limit_bytes=VMEM_LIMIT),
            name="sum_rows",
        )(upto, src, at, cnt, place, jnp.stack([tp % 2, jnp.int32(local)]), sums, *got)
        act_shape = (seqs, span, dim)
        return x_emb.reshape(act_shape), y_norm.reshape(act_shape), emb_grad, w_grad

    act_spec = P("dp", "tp", None)
    return jax.shard_map(local_step, mesh=mesh, in_specs=(P("dp", None), P("tp", None), P(None), act_spec, act_spec), out_specs=(act_spec, act_spec, P(("tp", "dp"), None), P(None)), check_vma=False)
```

```python
import functools
import math

import jax
import jax.numpy as jnp
import numpy as np
from jax import lax
from jax.experimental import pallas as pl
from jax.experimental.pallas import tpu as pltpu
from jax.sharding import PartitionSpec as P

NORM_EPS = 1e-6
LANES = 128
GATHER_ROWS = 16
GATHER_DEPTH = 6
SUM_DEPTH = 32
TOKEN_BLOCK = 128
TOKEN_GROUP = 16
OUT_BLOCK = 512
SUM_ROWS = 8
COPY_ROWS = 16
SIZES = (16, 32, 48, 64, 72, 80, 88, 96, 104, 112, 120, 128, 144, 160, 192, 224, 256, 288, 320, 352, 368, 384, 392, 400, 416, 432, 448, 456, 464, 480, 512, 544, 576, 640, 704, 768, 896)
VMEM_LIMIT = 60 * 1024 * 1024


def count_below(values, edges):
    return jnp.sum((values[:, :, None] < edges[None, None, :]).astype(jnp.int32), axis=1)


def chunk_table(starts, lens, size, most):
    per_run = (lens + size - 1) // size
    upto = jnp.cumsum(per_run)
    before = upto - per_run
    chunk = jnp.arange(most, dtype=jnp.int32)
    hit = (chunk[:, None] >= before[None, :]) & (chunk[:, None] < upto[None, :])
    done = size * (chunk[:, None] - before[None, :])
    cut = [jnp.sum(jnp.where(hit, start[None, :] + done, 0), axis=1) for start in starts]
    left = jnp.sum(jnp.where(hit, lens[None, :] - done, 0), axis=1)
    return cut, jnp.clip(left, 0, size), upto


def lookup_exchange_kernel(core, size, stride, most, sent_ref, got_ref, send_sems, recv_sems):
    tp = lax.axis_index("tp")
    mine = lax.rem(tp, 2)
    region = pl.ds((tp // 2) * most, size)

    def copy(hop):
        peer = tp + hop - 2 * (tp & hop)
        return pltpu.make_async_remote_copy(
            src_ref=sent_ref.at[pl.ds(peer * stride, size)],
            dst_ref=got_ref.at[region],
            send_sem=send_sems.at[hop - 1],
            recv_sem=recv_sems.at[hop - 1],
            device_id={"tp": peer},
            device_id_type=pl.DeviceIdType.MESH,
        )

    @pl.when(mine == core)
    def _():
        for hop in (2, 3, 1):
            copy(hop).start()
        for hop in (1, 2, 3):
            copy(hop).wait_send()
        copy(2).wait_recv()

    @pl.when(mine != core)
    def _():
        for hop in (1, 3):
            copy(hop).wait_recv()


def grad_exchange_kernel(core, size, stride, most, num_tp, sums_ref, w_ref, got_ref, wgot_ref, send_sems, recv_sems):
    dp, tp = lax.axis_index("dp"), lax.axis_index("tp")
    mine = lax.rem(tp, 2)
    me = dp * num_tp + tp

    def copies(hop_x, hop_y, source):
        peer_x = tp // 2 + hop_x - 2 * ((tp // 2) & hop_x)
        peer_tp = peer_x * 2 + core
        peer_dp = dp + hop_y - 2 * (dp & hop_y)
        refs = (
            (sums_ref.at[pl.ds((peer_tp * 2 + peer_dp) * stride, size)], got_ref.at[pl.ds(source * most, size)]),
            (w_ref, wgot_ref.at[source]),
        )
        return [
            pltpu.make_async_remote_copy(
                src_ref=src,
                dst_ref=dst,
                send_sem=send_sems.at[i, hop_y * 2 + hop_x],
                recv_sem=recv_sems.at[i, source],
                device_id={"dp": peer_dp, "tp": peer_tp},
                device_id_type=pl.DeviceIdType.MESH,
            )
            for i, (src, dst) in enumerate(refs)
        ]

    for hop_x, hop_y in ((1, 1), (1, 0), (0, 1)):
        for copy in copies(hop_x, hop_y, me):
            copy.start()

    @pl.when(mine != core)
    def _():
        for copy in copies(0, 0, me):
            copy.start()

    for hop_x, hop_y in ((1, 1), (1, 0), (0, 1)):
        for copy in copies(hop_x, hop_y, me):
            copy.wait_send()

    @pl.when(mine != core)
    def _():
        for copy in copies(0, 0, me):
            copy.wait_send()

    @pl.when(mine == core)
    def _():
        for source in range(2 * num_tp):

            @pl.when(source != me)
            def _():
                for copy in copies(1, 1, source):
                    copy.wait_recv()


def by_size(kernel, needed, sizes, shapes, name, sems, *operands):
    def branch(size):
        def call(*held):
            return pl.pallas_call(
                functools.partial(kernel, size),
                out_shape=[jax.ShapeDtypeStruct(shape, jnp.float32) for shape in shapes],
                in_specs=[pl.BlockSpec(memory_space=pl.ANY)] * len(held),
                out_specs=[pl.BlockSpec(memory_space=pl.ANY)] * len(shapes),
                scratch_shapes=[pltpu.SemaphoreType.DMA(sems[0]), pltpu.SemaphoreType.DMA(sems[1])],
                compiler_params=pltpu.CompilerParams(has_side_effects=True),
                name=f"{name}_{size}",
            )(*held)

        return call

    which = jnp.sum((needed > jnp.asarray(sizes, jnp.int32)).astype(jnp.int32))
    return lax.switch(which, [branch(size) for size in sizes], *operands)


def gather_kernel(scale, wide, row_ref, src_ref, dst_ref, num_ref, table_ref, out_ref, slots, spread, stage, in_sems, out_sems):
    num = num_ref[0]

    def fetch(chunk):
        slot = lax.rem(chunk, GATHER_DEPTH)
        src = src_ref[chunk]
        for i in range(GATHER_ROWS):
            first = pl.multiple_of((row_ref[src + i] // 8) * 8, 8)
            pltpu.make_async_copy(table_ref.at[pl.ds(first, 8), :], slots.at[slot, i], in_sems.at[slot]).start()

    def put(chunk):
        slot = lax.rem(chunk, 2)
        return pltpu.make_async_copy(stage.at[slot], out_ref.at[pl.ds(dst_ref[chunk], GATHER_ROWS)], out_sems.at[slot])

    def prime(chunk, _):
        fetch(chunk)
        return 0

    lax.fori_loop(0, jnp.minimum(num, GATHER_DEPTH - 1), prime, 0)

    def body(chunk, _):
        slot = lax.rem(chunk, GATHER_DEPTH)
        out_slot = lax.rem(chunk, 2)

        @pl.when(chunk + GATHER_DEPTH - 1 < num)
        def _():
            fetch(chunk + GATHER_DEPTH - 1)

        pltpu.make_async_copy(slots.at[slot], slots.at[slot], in_sems.at[slot]).wait()

        @pl.when(chunk >= 2)
        def _():
            put(chunk - 2).wait()

        src = src_ref[chunk]
        for i in range(GATHER_ROWS):
            for k in range(wide):
                spread[i, 8 * k : 8 * k + 8, :] = slots[slot, i, :, k * LANES : (k + 1) * LANES].astype(jnp.float32)
            row = lax.rem(row_ref[src + i], 8)
            stage[out_slot, i] = spread[i, pl.ds(row, wide, stride=8), :] * scale
        put(chunk).start()
        return 0

    lax.fori_loop(0, num, body, 0)

    @pl.when(num >= 2)
    def _():
        put(num - 2).wait()

    @pl.when(num >= 1)
    def _():
        put(num - 1).wait()


def token_kernel(wide, num_tp, most, stride, pos_ref, seg_ref, own_ref, sent_ref, got0_ref, got1_ref, w_ref, dyn_ref, dyr_ref, xe_ref, y_ref, sums_ref, wg_ref, held, total, grid_x, grid_g, wsum, sems):
    step = pl.program_id(0)
    steps = pl.num_programs(0)
    dim = wide * LANES
    num_own = 2 * num_tp

    def load_all(act):
        for p in range(num_tp):
            got = got1_ref if p % 2 else got0_ref

            def one(i, _):
                to = held.at[pl.ds(seg_ref[num_tp + p] + i * COPY_ROWS, COPY_ROWS)]

                @pl.when(own_ref[0] == p)
                def _():
                    act(pltpu.make_async_copy(sent_ref.at[pl.ds(p * stride + i * COPY_ROWS, COPY_ROWS)], to, sems.at[0]))

                @pl.when(own_ref[0] != p)
                def _():
                    act(pltpu.make_async_copy(got.at[pl.ds((p // 2) * most + i * COPY_ROWS, COPY_ROWS)], to, sems.at[0]))

                return 0

            lax.fori_loop(0, seg_ref[p], one, 0)

    def store_all(act):
        for o in range(num_own):

            def one(i, _):
                at = total.at[pl.ds(seg_ref[2 * num_tp + num_own + o] + i * COPY_ROWS, COPY_ROWS)]
                act(pltpu.make_async_copy(at, sums_ref.at[pl.ds(o * stride + i * COPY_ROWS, COPY_ROWS)], sems.at[0]))
                return 0

            lax.fori_loop(0, seg_ref[2 * num_tp + o], one, 0)

    @pl.when(step == 0)
    def _():
        load_all(lambda copy: copy.start())

        def clear(i, _):
            for j in range(8):
                total[i * 8 + j] = jnp.zeros((wide, LANES), jnp.float32)
            return 0

        lax.fori_loop(0, total.shape[0] // 8, clear, 0)
        wsum[...] = jnp.zeros_like(wsum)
        load_all(lambda copy: copy.wait())

    def group(index, _):
        base = step * TOKEN_BLOCK + index * TOKEN_GROUP
        rows = pl.ds(pl.multiple_of(index * TOKEN_GROUP, TOKEN_GROUP), TOKEN_GROUP)
        where = [pos_ref[base + j] for j in range(TOKEN_GROUP)]
        for j in range(TOKEN_GROUP):
            grid_x[pl.ds(j, wide, stride=TOKEN_GROUP), :] = held[where[j]]
        tile = [slice(TOKEN_GROUP * k, TOKEN_GROUP * (k + 1)) for k in range(wide)]
        lane = [slice(LANES * k, LANES * (k + 1)) for k in range(wide)]
        square = jnp.zeros((TOKEN_GROUP, LANES), jnp.float32)
        for k in range(wide):
            xe = grid_x[tile[k], :].astype(jnp.bfloat16)
            xe_ref[rows, lane[k]] = xe
            x = xe.astype(jnp.float32)
            grid_x[tile[k], :] = x
            square += x * x
        inv = lax.rsqrt(jnp.sum(square, axis=1, keepdims=True) * (1.0 / dim) + NORM_EPS)
        inner = jnp.zeros((TOKEN_GROUP, LANES), jnp.float32)
        for k in range(wide):
            xh = grid_x[tile[k], :] * inv
            grid_x[tile[k], :] = xh
            gain = 1.0 + w_ref[0:1, lane[k]]
            inner += dyn_ref[rows, lane[k]].astype(jnp.float32) * gain * xh
        mean = jnp.sum(inner, axis=1, keepdims=True) * (1.0 / dim)
        for k in range(wide):
            xh = grid_x[tile[k], :]
            gain = 1.0 + w_ref[0:1, lane[k]]
            dy = dyn_ref[rows, lane[k]].astype(jnp.float32)
            y_ref[rows, lane[k]] = (xh * gain).astype(jnp.bfloat16)
            wsum[:, lane[k]] += dy * xh
            grid_g[tile[k], :] = dyr_ref[rows, lane[k]].astype(jnp.float32) + inv * (dy * gain - xh * mean)
        for j in range(TOKEN_GROUP):
            total[where[j]] += grid_g[pl.ds(j, wide, stride=TOKEN_GROUP), :]
        return 0

    lax.fori_loop(0, TOKEN_BLOCK // TOKEN_GROUP, group, 0)

    @pl.when(step == steps - 1)
    def _():
        for k in range(wide):
            wg_ref[k : k + 1, :] = jnp.sum(wsum[:, LANES * k : LANES * (k + 1)], axis=0, keepdims=True)
        store_all(lambda copy: copy.start())
        store_all(lambda copy: copy.wait())


def sum_kernel(scale, wide, depth, upto_ref, src_ref, at_ref, cnt_ref, place_ref, own_ref, sums_ref, got0_ref, got1_ref, out_ref, acc, ring, sems):
    block = pl.program_id(0)
    num = upto_ref[pl.num_programs(0)]
    spare = (OUT_BLOCK // 8) * wide * 8

    def fetch(chunk):
        slot = lax.rem(chunk, depth)
        src = src_ref[chunk]

        @pl.when(src < own_ref[1])
        def _():
            @pl.when(own_ref[0] == 0)
            def _():
                pltpu.make_async_copy(got0_ref.at[pl.ds(src, SUM_ROWS)], ring.at[slot], sems.at[slot]).start()

            @pl.when(own_ref[0] != 0)
            def _():
                pltpu.make_async_copy(got1_ref.at[pl.ds(src, SUM_ROWS)], ring.at[slot], sems.at[slot]).start()

        @pl.when(src >= own_ref[1])
        def _():
            pltpu.make_async_copy(sums_ref.at[pl.ds(src - own_ref[1], SUM_ROWS)], ring.at[slot], sems.at[slot]).start()

    @pl.when(block == 0)
    def _():
        def prime(chunk, _):
            fetch(chunk)
            return 0

        lax.fori_loop(0, jnp.minimum(num, depth - 1), prime, 0)

        def clear(i, _):
            acc[pl.ds(pl.multiple_of(i * wide * 8, 8), wide * 8), :] = jnp.zeros((wide * 8, LANES), jnp.float32)
            return 0

        lax.fori_loop(0, OUT_BLOCK // 8 + 1, clear, 0)

    def body(chunk, _):
        slot = lax.rem(chunk, depth)
        pltpu.make_async_copy(got0_ref.at[pl.ds(0, SUM_ROWS)], ring.at[slot], sems.at[slot]).wait()

        @pl.when(chunk + depth - 1 < num)
        def _():
            fetch(chunk + depth - 1)

        src, cnt = at_ref[chunk], cnt_ref[chunk]
        at = [pl.ds(jnp.where(i < cnt, place_ref[src + i], spare), wide, stride=8) for i in range(SUM_ROWS)]
        summed = [acc[at[i], :] + ring[slot, i] for i in range(SUM_ROWS)]
        for i in range(SUM_ROWS):
            acc[at[i], :] = summed[i]
        return 0

    lax.fori_loop(upto_ref[block], upto_ref[block + 1], body, 0)

    def put(i, _):
        rows = pl.ds(pl.multiple_of(i * 8, 8), 8)
        for k in range(wide):
            at = pl.ds(pl.multiple_of(i * wide * 8 + 8 * k, 8), 8)
            out_ref[rows, k * LANES : (k + 1) * LANES] = acc[at, :] * scale
            acc[at, :] = jnp.zeros((8, LANES), jnp.float32)
        return 0

    lax.fori_loop(0, OUT_BLOCK // 8, put, 0)


def solution(mesh):
    num_dp, num_tp = mesh.shape["dp"], mesh.shape["tp"]
    num_dev = num_dp * num_tp

    def local_step(tokens, emb_table, w_norm, dy_norm, dy_resid):
        shard_rows, dim = emb_table.shape
        seqs, span = dy_norm.shape[:2]
        held_rows = seqs * span
        wide = dim // LANES
        vocab = shard_rows * num_tp
        own_rows = shard_rows // num_dp
        scale = float(np.float32(math.sqrt(dim)).astype(jnp.bfloat16))
        dp, tp = lax.axis_index("dp"), lax.axis_index("tp")
        any_space = pl.BlockSpec(memory_space=pl.ANY)
        smem = pl.BlockSpec(memory_space=pltpu.SMEM)

        my_ids = lax.dynamic_slice_in_dim(tokens, tp * span, span, 1).reshape(held_rows)
        turn = jnp.arange(held_rows, dtype=jnp.int32)
        again = (my_ids[None, :] == my_ids[:, None]) & (turn[None, :] < turn[:, None])
        first = jnp.logical_not(jnp.any(again, axis=1))
        place = jnp.sum((first[None, :] & (my_ids[None, :] < my_ids[:, None])).astype(jnp.int32), axis=1)
        my_uniq = jnp.min(jnp.where(place[None, :] == turn[:, None], my_ids[None, :], vocab), axis=1)
        uniq = lax.all_gather(my_uniq[None], ("dp", "tp"), axis=0, tiled=True)
        edges = jnp.arange(num_dev + 1, dtype=jnp.int32) * own_rows
        cuts = count_below(uniq, edges)
        shard_cuts = cuts[:, ::num_dp]
        me, own = dp * num_tp + tp, tp * num_dp + dp
        device = jnp.arange(num_dev, dtype=jnp.int32)

        looked = shard_cuts[:, 1:] - shard_cuts[:, :-1]
        looked = jnp.where(jnp.arange(num_tp)[None, :] == (device % num_tp)[:, None], 0, looked)
        owned = cuts[:, 1:] - cuts[:, :-1]
        owned = jnp.where(device[None, :] == ((device % num_tp) * num_dp + device // num_tp)[:, None], 0, owned)
        look_need = [jnp.max(looked[:, core::2]) for core in range(2)]
        grad_need = [jnp.max(owned.reshape(num_dev, num_tp, num_dp)[:, core::2]) for core in range(2)]
        sizes = [size for size in SIZES if size < held_rows] + [held_rows]

        group = dp * num_tp + jnp.arange(num_tp, dtype=jnp.int32)
        group_cuts = lax.dynamic_slice_in_dim(shard_cuts, dp * num_tp, num_tp, 0)
        lo = lax.dynamic_index_in_dim(group_cuts, tp, 1, keepdims=False)
        size = lax.dynamic_index_in_dim(group_cuts, tp + 1, 1, keepdims=False) - lo
        stride = held_rows + GATHER_ROWS
        most = num_tp * (held_rows // GATHER_ROWS) + num_tp
        lane_of = jnp.arange(num_tp, dtype=jnp.int32)
        (src, dst), _, upto = chunk_table([group * held_rows + lo, lane_of * stride], size, GATHER_ROWS, most)
        listed = jnp.clip(uniq - tp * shard_rows, 0, shard_rows - 1).reshape(-1)
        listed = jnp.pad(listed, (0, GATHER_ROWS))
        sent = pl.pallas_call(
            functools.partial(gather_kernel, scale, wide),
            out_shape=jax.ShapeDtypeStruct((num_tp * stride, wide, LANES), jnp.float32),
            in_specs=[smem] * 4 + [any_space],
            out_specs=any_space,
            scratch_shapes=[
                pltpu.VMEM((GATHER_DEPTH, GATHER_ROWS, 8, dim), jnp.bfloat16),
                pltpu.VMEM((GATHER_ROWS, wide * 8, LANES), jnp.float32),
                pltpu.VMEM((2, GATHER_ROWS, wide, LANES), jnp.float32),
                pltpu.SemaphoreType.DMA((GATHER_DEPTH,)),
                pltpu.SemaphoreType.DMA((2,)),
            ],
            compiler_params=pltpu.CompilerParams(vmem_limit_bytes=16 * 1024 * 1024),
            name="gather",
        )(listed, src, dst, upto[-1:], emb_table)
        rows = []
        for core in range(2):

            def look(size, *refs, core=core):
                lookup_exchange_kernel(core, size, stride, held_rows, *refs)

            shape = (num_tp // 2 * held_rows, wide, LANES)
            rows += by_size(look, look_need[core], sizes, [shape], f"lookup{core}", ((3,), (3,)), sent)

        my_cuts = lax.dynamic_index_in_dim(cuts, me, 0, keepdims=False)
        seg_lo = my_cuts[:-1:num_dp]
        seg_copies = (my_cuts[num_dp::num_dp] - seg_lo + COPY_ROWS - 1) // COPY_ROWS
        seg_base = (jnp.cumsum(seg_copies) - seg_copies) * COPY_ROWS
        shift = seg_base - seg_lo
        pos = place + jnp.sum(jnp.where((my_ids // shard_rows)[:, None] == lane_of[None, :], shift[None, :], 0), axis=1)
        own_copies = (my_cuts[1:] - my_cuts[:-1] + COPY_ROWS - 1) // COPY_ROWS
        own_base = my_cuts[:-1] + jnp.repeat(shift, num_dp)
        segments = jnp.concatenate([seg_copies, seg_base, own_copies, own_base])
        token_spec = pl.BlockSpec((TOKEN_BLOCK, dim), lambda i: (i, 0))
        act = jax.ShapeDtypeStruct((held_rows, dim), jnp.bfloat16)
        kept = held_rows + (num_tp + 1) * COPY_ROWS
        x_emb, y_norm, sums, w_part = pl.pallas_call(
            functools.partial(token_kernel, wide, num_tp, held_rows, stride),
            grid=(held_rows // TOKEN_BLOCK,),
            out_shape=[act, act, jax.ShapeDtypeStruct((num_dev * stride, wide, LANES), jnp.float32), jax.ShapeDtypeStruct((wide, LANES), jnp.float32)],
            in_specs=[smem] * 3 + [any_space] * 3 + [pl.BlockSpec((1, dim), lambda i: (0, 0)), token_spec, token_spec],
            out_specs=[token_spec, token_spec, any_space, pl.BlockSpec((wide, LANES), lambda i: (0, 0))],
            scratch_shapes=[
                pltpu.VMEM((kept, wide, LANES), jnp.float32),
                pltpu.VMEM((kept, wide, LANES), jnp.float32),
                pltpu.VMEM((TOKEN_GROUP * wide, LANES), jnp.float32),
                pltpu.VMEM((TOKEN_GROUP * wide, LANES), jnp.float32),
                pltpu.VMEM((TOKEN_GROUP, dim), jnp.float32),
                pltpu.SemaphoreType.DMA((1,)),
            ],
            compiler_params=pltpu.CompilerParams(vmem_limit_bytes=VMEM_LIMIT),
            name="tokens",
        )(pos, segments, tp.reshape(1), sent, *rows, w_norm.reshape(1, dim), dy_norm.reshape(held_rows, dim), dy_resid.reshape(held_rows, dim))
        got = []
        for core in range(2):

            def give(size, *refs, core=core):
                grad_exchange_kernel(core, size, stride, held_rows, num_tp, *refs)

            shapes = [(num_dev * held_rows + SUM_ROWS, wide, LANES), (num_dev, wide, LANES)]
            got.append(by_size(give, grad_need[core], sizes, shapes, f"grads{core}", ((2, 4), (2, num_dev)), sums, w_part))

        w_all = jnp.where(tp % 2 == 0, got[0][1], got[1][1])
        w_grad = jnp.sum(jnp.where((device == me)[:, None, None], w_part[None], w_all), axis=0).reshape(dim)

        blocks = own_rows // OUT_BLOCK
        marks = own * own_rows + jnp.arange(blocks + 1, dtype=jnp.int32) * OUT_BLOCK
        fence = count_below(uniq, marks)
        local = num_dev * held_rows + SUM_ROWS
        first = jnp.where(device == me, local + own * stride, device * held_rows)
        run_at = (device[:, None] * held_rows + fence[:, :-1]).T.reshape(-1)
        run_src = (first[:, None] + fence[:, :-1] - fence[:, :1]).T.reshape(-1)
        run_len = (fence[:, 1:] - fence[:, :-1]).T.reshape(-1)
        most = num_dev * held_rows // SUM_ROWS + blocks * num_dev
        (src, at), cnt, upto = chunk_table([run_src, run_at], run_len, SUM_ROWS, most)
        upto = jnp.concatenate([jnp.zeros((1,), jnp.int32), upto[num_dev - 1 :: num_dev]])
        inside = uniq.reshape(-1) & (OUT_BLOCK - 1)
        place = jnp.pad((inside >> 3) * (wide * 8) + (inside & 7), (0, SUM_ROWS))
        depth = SUM_DEPTH
        emb_grad = pl.pallas_call(
            functools.partial(sum_kernel, scale, wide, depth),
            grid=(blocks,),
            out_shape=jax.ShapeDtypeStruct((own_rows, dim), jnp.float32),
            in_specs=[smem] * 6 + [any_space] * 3,
            out_specs=pl.BlockSpec((OUT_BLOCK, dim), lambda i: (i, 0)),
            scratch_shapes=[
                pltpu.VMEM(((OUT_BLOCK // 8 + 1) * wide * 8, LANES), jnp.float32),
                pltpu.VMEM((depth, SUM_ROWS, wide, LANES), jnp.float32),
                pltpu.SemaphoreType.DMA((depth,)),
            ],
            compiler_params=pltpu.CompilerParams(vmem_limit_bytes=VMEM_LIMIT),
            name="sum_rows",
        )(upto, src, at, cnt, place, jnp.stack([tp % 2, jnp.int32(local)]), sums, got[0][0], got[1][0])
        act_shape = (seqs, span, dim)
        return x_emb.reshape(act_shape), y_norm.reshape(act_shape), emb_grad, w_grad

    act_spec = P("dp", "tp", None)
    return jax.shard_map(local_step, mesh=mesh, in_specs=(P("dp", None), P("tp", None), P(None), act_spec, act_spec), out_specs=(act_spec, act_spec, P(("tp", "dp"), None), P(None)), check_vma=False)
```
